32 devices in a mesh: scene: 2 (over x), along: 16 (over z, y, core).
Axes of the slice: x: 2, y: 2, z: 4, core: 2. Of those that a mesh axis runs over, the one named last changes fastest.
Arguments:
- echoes: bfloat16 [2, 64, 16, 16, 256], P(None, ('scene', 'along')), parts along dimension 1, may hold values from -6 to 6
- integer_cell_displacement: int32 [64, 16], P(('scene', 'along')), parts along dimension 0, may hold values from 0 to 15
- fractional_level_label: int32 [64, 16], P(('scene', 'along')), parts along dimension 0, may hold values from 0 to 15
- steering: bfloat16 [2, 256, 256], replicated, may hold values from -0.25 to 0.25
- tile_anchor: int32 [32], P('scene'), parts along dimension 0, may hold values from -64 to 3904, as said below
Outputs:
- image_tiles: bfloat16 [2, 8192, 256], P(None, ('scene', 'along')), parts along dimension 1
The draws below stay inside these ranges and needn't reach their ends.
There are 2 independent parts, one for each index of `scene`. The reference program is written for one: setup_inputs(seed, part) draws one part's arguments, and reference() takes and returns one part's arrays. A program takes and returns all parts, laid end to end along the dimension named above; an argument that names none is the same for every part. Nothing has to cross between parts.
Inputs may be any that keep to these rules, and one draw needn't show every extreme that they name: tile_anchor[j] lies within 64 of j * 256.
All inputs are finite; a program needn't handle non-finite values.
Results may differ from the reference program's by a relative error of at most 0.0064.
Values may be sent and summed in bfloat16 or wider, within the bound.
No kernel may reach another device: no remote copies, remote signals or barrier semaphores. Data moves between devices by JAX's collectives and lax.ppermute only.
A program may use at most 64 MiB of HBM per device.

```python
import math
import jax
import jax.numpy as jnp
from jax import lax

TX = 16
RX = 16
BEAMS = 256
BINS = 256
PULSE_DEV = 2
TILE_X = 256
STEPS = 16
TAPS = 8
SHIFTS = 16
FRACTION_LEVELS = 16
QUAD = 4093
WAVE_FOURTHS = 37
CHANS = 256
ECHO_TOTAL = 32
TILES = 16


def draw_tile_anchor(key, part):
    jitter = jax.random.randint(jax.random.fold_in(key, 7), (TILES,), -(TILE_X // 4), TILE_X // 4 + 1)
    return (jnp.arange(TILES, dtype=jnp.int32) * TILE_X + jitter).astype(jnp.int32)


def set_ends(array, rng, low, largest):
    longest = array.shape.index(max(array.shape))
    spots = []
    for shift in (0, 1):
        where = [jax.random.randint(jax.random.fold_in(rng, axis), (), 0, length) for axis, length in enumerate(array.shape)]
        where[longest] = (where[longest] + shift) % array.shape[longest]
        spots.append(tuple(where))
    return array.at[spots[0]].set(low).at[spots[1]].set(largest)


def block_scale(key, shape, shards, low, largest):
    def one(position, blocks):
        heights = jax.random.uniform(jax.random.fold_in(jax.random.fold_in(key, 6), position), (blocks,), jnp.float32, low / len(shards), largest / len(shards))
        return jnp.repeat(jnp.exp(heights), shape[position] // blocks).reshape((-1,) + (1,) * (len(shape) - position - 1))

    loudness = one(*shards[0])
    for cut in shards[1:]:
        loudness = loudness * one(*cut)
    return loudness


def noise(key, extent, spread, bound, split=(), kind=jnp.bfloat16):
    gain = block_scale(key, extent, split, -0.22, 0.18) if split else 1.0
    entries = jax.random.normal(key, extent, jnp.float32) * spread * gain
    return jnp.minimum(jnp.maximum(entries, -bound), bound).astype(kind)


def setup_inputs(seed: int = 0, part: int = 0) -> dict:
    seeds = jax.random.split(jax.random.key(seed), 6)
    own_keys = jax.random.split(jax.random.fold_in(seeds[5], part), 6)
    echoes = noise(own_keys[0], (2, ECHO_TOTAL, TX, RX, BINS), 1.0, 6.0, ((1, 16),))
    integer_cell_displacement = set_ends(jax.random.randint(own_keys[1], (ECHO_TOTAL, TX), 0, SHIFTS), jax.random.fold_in(own_keys[1], 1), 0, SHIFTS - 1).astype(jnp.int32)
    fractional_level_label = set_ends(jax.random.randint(own_keys[2], (ECHO_TOTAL, TX), 0, FRACTION_LEVELS), jax.random.fold_in(own_keys[2], 1), 0, FRACTION_LEVELS - 1).astype(jnp.int32)
    steering = noise(seeds[3], (2, CHANS, BEAMS), (2 * CHANS) ** -0.5, 0.25)
    tile_anchor = draw_tile_anchor(jax.random.fold_in(jax.random.fold_in(seeds[5], part), 71), part)
    return dict(echoes=echoes, integer_cell_displacement=integer_cell_displacement, fractional_level_label=fractional_level_label, steering=steering, tile_anchor=tile_anchor)


def tap_weights(integer_cell_displacement, fractional_level_label):
    fraction = fractional_level_label.astype(jnp.float32) / FRACTION_LEVELS
    tap_place = jnp.arange(TAPS, dtype=jnp.float32) - (TAPS // 2 - 1)
    displacement = tap_place[None, None, :] - fraction[..., None]
    window_taper = 0.54 + 0.46 * jnp.cos(math.pi * displacement / (TAPS // 2))
    kernel = jnp.sinc(displacement) * window_taper
    angle_turns = jnp.mod(WAVE_FOURTHS * (integer_cell_displacement * FRACTION_LEVELS + fractional_level_label), 4 * FRACTION_LEVELS).astype(jnp.float32) / (4 * FRACTION_LEVELS)
    phase_angle = 2.0 * math.pi * angle_turns
    return kernel * jnp.cos(phase_angle)[..., None], -kernel * jnp.sin(phase_angle)[..., None]


def compensate(echoes, integer_cell_displacement, fractional_level_label):
    bin_count = echoes.shape[-1]
    margin = SHIFTS // 2 + TAPS // 2
    padded = jnp.pad(echoes, ((0, 0), (0, 0), (0, 0), (0, 0), (margin, margin)))
    starts = (margin + integer_cell_displacement - SHIFTS // 2 - (TAPS // 2 - 1)).astype(jnp.int32)
    span_cells = bin_count + TAPS - 1

    def take_window(pulse_block, start):
        return lax.dynamic_slice_in_dim(pulse_block, start, span_cells, 2)

    windows = jax.vmap(jax.vmap(take_window, in_axes=(1, 0), out_axes=1), in_axes=(1, 0), out_axes=1)(padded, starts)
    coef_real, coef_imag = tap_weights(integer_cell_displacement, fractional_level_label)
    real_part = None
    imag_part = None
    for tap_index in range(TAPS):
        window_part = windows[..., tap_index:tap_index + bin_count]
        weight_real = coef_real[:, :, tap_index][:, :, None, None]
        weight_imag = coef_imag[:, :, tap_index][:, :, None, None]
        add_real = weight_real * window_part[0] - weight_imag * window_part[1]
        add_imag = weight_real * window_part[1] + weight_imag * window_part[0]
        real_part = add_real if real_part is None else real_part + add_real
        imag_part = add_imag if imag_part is None else imag_part + add_imag
    return jnp.stack([real_part, imag_part]).astype(jnp.bfloat16)


def form_beams(compensated, steering):
    pulse_count = compensated.shape[1]
    bin_count = compensated.shape[4]
    count_of_beams = steering.shape[2]
    flat_comp = compensated.reshape(2, pulse_count, -1, bin_count)
    mixer_grid = jnp.stack([jnp.concatenate([steering[0], steering[1]], 1),
                            jnp.concatenate([-steering[1], steering[0]], 1)])
    formed = jnp.einsum("pkcw,pcq->qkw", flat_comp.astype(jnp.float32), mixer_grid.astype(jnp.float32))
    return formed.reshape(2, count_of_beams, pulse_count, bin_count).astype(jnp.bfloat16)


def phase_table(count_of_beams, pulse_count, source, anchor):
    pulse_numbers = jnp.arange(pulse_count, dtype=jnp.int32)
    pixels = jnp.arange(TILE_X, dtype=jnp.int32)
    pixel_ratio = TILE_X // pulse_count
    pulse_spot = (source * pulse_count + pulse_numbers) * pixel_ratio
    offset_cells = anchor + pixels[None, :] - pulse_spot[:, None]
    beam_ids = jnp.arange(count_of_beams, dtype=jnp.int32)
    displacement_residue = jnp.mod(offset_cells, QUAD).astype(jnp.int32)
    offset_square = jnp.mod(displacement_residue * displacement_residue, QUAD).astype(jnp.int32)
    beam_square = jnp.mod(beam_ids * beam_ids, QUAD).astype(jnp.int32)
    phase_units = jnp.mod(offset_square[None] + beam_square[:, None, None] * displacement_residue[None]
                          + beam_ids[:, None, None] * offset_square[None], QUAD).astype(jnp.int32)
    phase_angle = 2.0 * math.pi * (phase_units.astype(jnp.float32) / QUAD)
    gain_norm = (STEPS * pulse_count * count_of_beams) ** -0.5
    grid_real = (gain_norm * jnp.cos(phase_angle)).astype(jnp.bfloat16)
    grid_imag = (gain_norm * jnp.sin(phase_angle)).astype(jnp.bfloat16)
    return jnp.stack([jnp.concatenate([grid_real, grid_imag], -1),
                      jnp.concatenate([-grid_imag, grid_real], -1)])


def project(beam_data, source, anchor):
    phase_grid = phase_table(beam_data.shape[1], beam_data.shape[2], source, anchor)
    summed = jnp.einsum("pakq,pakw->qw", phase_grid.astype(jnp.float32), beam_data.astype(jnp.float32))
    return summed.reshape(2, TILE_X, beam_data.shape[3])


def reference(echoes, integer_cell_displacement, fractional_level_label, steering, tile_anchor):
    beam_data = form_beams(compensate(echoes, integer_cell_displacement, fractional_level_label), steering)

    def one_tile(tile_id):
        running = jnp.zeros((2, TILE_X, BINS), jnp.float32)
        for distance in range(STEPS):
            source = tile_id - distance
            inside = source >= 0
            clamped = jnp.maximum(source, 0).astype(jnp.int32)
            pulse_block = lax.dynamic_slice_in_dim(beam_data, clamped * PULSE_DEV, PULSE_DEV, 2)
            contrib = project(pulse_block, clamped, tile_anchor[tile_id])
            running = running + jnp.where(inside, contrib, jnp.zeros_like(contrib))
        return running

    tile_sums = lax.map(one_tile, jnp.arange(TILES, dtype=jnp.int32))
    image_tiles = tile_sums.transpose(1, 0, 2, 3).reshape(2, TILES * TILE_X, BINS)
    return image_tiles.astype(jnp.bfloat16)
```

```python
import math

import jax
import jax.numpy as jnp
import numpy as np
from jax import lax
from jax.experimental import pallas as pl
from jax.experimental.pallas import tpu as pltpu
from jax.sharding import PartitionSpec as P

TILE_X = 256
STEPS = 16
TAPS = 8
SHIFTS = 16
FRACTION_LEVELS = 16
QUAD = 4093
WAVE_FOURTHS = 37
LANES = 128
FIRST_BLOCK = -2
UNITS = STEPS + 2
F32 = jnp.float32
BF16 = jnp.bfloat16


def filter_tables():
    fraction = np.arange(FRACTION_LEVELS)[:, None] / FRACTION_LEVELS
    place = np.arange(TAPS)[None, :] - (TAPS // 2 - 1) - fraction
    kernel = np.sinc(place) * (0.54 + 0.46 * np.cos(np.pi * place / (TAPS // 2)))
    angle = 2 * np.pi * np.arange(4 * FRACTION_LEVELS) / (4 * FRACTION_LEVELS)
    turn = np.stack([np.cos(angle), np.sin(angle)])
    return kernel.reshape(-1).astype(np.float32), turn.reshape(-1).astype(np.float32)


def circle_series():
    angle = np.cos(np.linspace(0, np.pi, 4001)) * np.pi
    odd = np.stack([angle ** (2 * k + 1) for k in range(6)], 1)
    even = np.stack([angle ** (2 * k) for k in range(7)], 1)
    sine = np.linalg.lstsq(odd, np.sin(angle), rcond=None)[0]
    cosine = np.linalg.lstsq(even, np.cos(angle), rcond=None)[0]
    return [float(c) for c in sine], [float(c) for c in cosine]


def horner(series, value):
    total = series[-1]
    for c in reversed(series[:-1]):
        total = total * value + c
    return total


def compensate_kernel(cells, levels, kernel_table, turn_table, echo, out, scratch, *, pulses, tx, rx, bins, split):
    lane = lax.broadcasted_iota(jnp.int32, (8, LANES), 1)
    groups = rx // 8

    def one(index, pulse):
        t = index
        cell = cells[pulse * tx + t]
        level = levels[pulse * tx + t]
        turns = jnp.bitwise_and(WAVE_FOURTHS * (cell * FRACTION_LEVELS + level), 4 * FRACTION_LEVELS - 1)
        turn_cos = turn_table[turns]
        turn_sin = turn_table[4 * FRACTION_LEVELS + turns]
        parts = [echo[c, pulse, t].astype(F32) for c in range(2)]
        rows = jnp.concatenate(parts, 0).reshape(2 * groups, 8, bins)
        low = rows[:, :, :LANES].reshape(16 * groups, LANES)
        high = rows[:, :, LANES:].reshape(16 * groups, LANES)
        sum_low = None
        for tap in range(TAPS):
            weight = kernel_table[level * TAPS + tap]
            shift = cell - SHIFTS // 2 - (TAPS // 2 - 1) + tap
            amount = jnp.bitwise_and(-shift, LANES - 1)
            moved_low = pltpu.roll(low, amount, 1).reshape(2 * groups, 8, LANES)
            moved_high = pltpu.roll(high, amount, 1).reshape(2 * groups, 8, LANES)
            at = lane + shift
            inside = (at >= 0) & (at < LANES)
            weight_low = jnp.where(at >= 0, weight, 0.0)
            weight_high = jnp.where(at < LANES, weight, 0.0)
            add_low = jnp.where(inside[None], moved_low, moved_high) * weight_low[None]
            add_high = jnp.where(inside[None], moved_high, moved_low) * weight_high[None]
            sum_low = add_low if sum_low is None else sum_low + add_low
            sum_high = add_high if tap == 0 else sum_high + add_high
        for half, total in enumerate((sum_low, sum_high)):
            real = total[:groups] * turn_cos + total[groups:] * turn_sin
            imag = total[groups:] * turn_cos - total[:groups] * turn_sin
            at_rows = pl.ds(pl.multiple_of(t * rx, rx), rx)
            at_lanes = slice(half * LANES, (half + 1) * LANES)
            scratch[0, pulse, at_rows, at_lanes] = real.reshape(rx, LANES)
            scratch[1, pulse, at_rows, at_lanes] = imag.reshape(rx, LANES)

    for pulse in range(pulses):
        def body(index, carry, pulse=pulse):
            one(index, pulse)
            return carry

        lax.fori_loop(0, tx, body, 0)
        for c in range(2):
            turned = jnp.transpose(scratch[c, pulse]).astype(BF16)
            at_lanes = slice(c * tx * rx, (c + 1) * tx * rx)
            if split:
                out[:, pulse, :, at_lanes] = turned.reshape(split, bins // split, tx * rx)
            else:
                out[pulse, :, at_lanes] = turned


def compensate(echoes, cells, levels, devices):
    _, pulses, tx, rx, bins = echoes.shape
    width = bins // devices
    chans = tx * rx
    split = devices if width % 16 == 0 else 0
    shape = (devices, pulses, width, 2 * chans) if split else (pulses, bins, 2 * chans)
    kernel_table, turn_table = filter_tables()
    smem = pl.BlockSpec(memory_space=pltpu.SMEM)

    def kernel(*refs):
        compensate_kernel(*refs, pulses=pulses, tx=tx, rx=rx, bins=bins, split=split)

    done = pl.pallas_call(
        kernel,
        out_shape=jax.ShapeDtypeStruct(shape, BF16),
        in_specs=[smem, smem, smem, smem, pl.BlockSpec(memory_space=pltpu.VMEM)],
        out_specs=pl.BlockSpec(memory_space=pltpu.VMEM),
        scratch_shapes=[pltpu.VMEM((2, pulses, chans, bins), F32)],
        name="compensate",
    )(cells.reshape(-1), levels.reshape(-1), jnp.asarray(kernel_table), jnp.asarray(turn_table), echoes)
    if not split:
        done = done.reshape(pulses, devices, width, 2 * chans).transpose(1, 0, 2, 3)
    return done


def table_kernel(steering, table, mixer, beam_square, beam_next, *, beams, gain):
    chans = steering.shape[1]
    real, imag = steering[0], steering[1]
    mixer[:chans, :beams] = real
    mixer[:chans, beams:] = imag
    mixer[chans:, :beams] = -imag
    mixer[chans:, beams:] = real
    sine, cosine = circle_series()
    sine = [c * gain for c in sine]
    cosine = [c * gain for c in cosine]

    def centred(value):
        return value - jnp.round(value * (1.0 / QUAD)) * float(QUAD)

    beam = lax.broadcasted_iota(jnp.int32, (beams, LANES), 0).astype(F32)
    beam_square[...] = centred(beam * beam)
    beam_next[...] = beam + 1.0
    step = 32

    def chunk(index, carry):
        offset = lax.broadcasted_iota(jnp.int32, (8, LANES), 1) + (index + FIRST_BLOCK) * LANES
        offset = centred(offset.astype(F32))
        square = centred(offset * offset)
        at_lanes = pl.ds(pl.multiple_of(index * LANES, LANES), LANES)
        for row in range(0, beams, step):
            at = slice(row, row + step)
            square_part = beam_square[at, :].reshape(step // 8, 8, LANES)
            next_part = beam_next[at, :].reshape(step // 8, 8, LANES)
            units = centred(square[None] * next_part + square_part * offset[None])
            angle = units * (2.0 * math.pi / QUAD)
            power = angle * angle
            table_cos = horner(cosine, power)
            table_sin = horner(sine, power) * angle
            table[row : row + step, at_lanes] = table_cos.reshape(step, LANES).astype(BF16)
            table[beams + row : beams + row + step, at_lanes] = table_sin.reshape(step, LANES).astype(BF16)
        return carry

    lax.fori_loop(0, 2 * UNITS, chunk, 0)


def make_table(steering, pulses):
    _, chans, beams = steering.shape
    gain = (STEPS * pulses * beams) ** -0.5

    def kernel(*refs):
        table_kernel(*refs, beams=beams, gain=gain)

    return pl.pallas_call(
        kernel,
        out_shape=(
            jax.ShapeDtypeStruct((2 * beams, 2 * UNITS * LANES), BF16),
            jax.ShapeDtypeStruct((2 * chans, 2 * beams), BF16),
        ),
        in_specs=[pl.BlockSpec(memory_space=pltpu.VMEM)],
        out_specs=(pl.BlockSpec(memory_space=pltpu.VMEM), pl.BlockSpec(memory_space=pltpu.VMEM)),
        scratch_shapes=[pltpu.VMEM((beams, LANES), F32), pltpu.VMEM((beams, LANES), F32)],
        cost_estimate=pl.CostEstimate(flops=40 * beams * 2 * UNITS * LANES * 1000, transcendentals=0, bytes_accessed=0),
        name="table",
    )(steering)


def project_kernel(anchors, data, mixer, table, out, left, right, common, edge_first, edge_low, edge_high, edge_last,
                   *, pulses, tiles, width, beams):
    rows = pulses * width
    formed = jnp.dot(data[...], mixer[...], preferred_element_type=F32)
    real = formed[:, :beams].astype(BF16)
    imag = formed[:, beams:].astype(BF16)
    left[:, :beams] = real
    left[:, beams:] = -imag
    right[:, :beams] = imag
    right[:, beams:] = real
    last_block = 2 * tiles

    def used(first):
        count = min(pulses, last_block - first + 1)
        return count, min(rows, -(-count * width // 16) * 16)

    def product(first, count):
        unit = (first - FIRST_BLOCK) // 2
        part = table[:, unit * 2 * LANES : (unit + 1) * 2 * LANES]
        return [jnp.dot(side[:count, :], part, preferred_element_type=F32) for side in (left, right)]

    for c, value in enumerate(product(0, rows)):
        edge_low[c, :rows, :] = value[:, :LANES]
        common[c, :rows, :LANES] = jnp.zeros((rows, LANES), F32)
        common[c, :rows, LANES:] = value[:, LANES:]
        common[c, rows:, :] = jnp.zeros((common.shape[1] - rows, 2 * LANES), F32)
    for c, value in enumerate(product(FIRST_BLOCK, rows)):
        edge_first[c] = value
    for first in range(2, 2 * STEPS - 2, 2):
        if first > last_block:
            break
        _, count = used(first)
        for c, value in enumerate(product(first, count)):
            at = slice(first * width, first * width + count)
            common[c, at, :] = common[c, at, :] + value
    for first, edge in ((2 * STEPS - 2, edge_high), (2 * STEPS, edge_last)):
        if first <= last_block:
            _, count = used(first)
            for c, value in enumerate(product(first, count)):
                edge[c, :count, :] = value

    lane = lax.broadcasted_iota(jnp.int32, (1, LANES), 1)

    def take(source, c, block, first, half):
        pulse = block - first
        if first > last_block or not 0 <= pulse < pulses:
            return []
        lanes = slice(half * LANES, (half + 1) * LANES)
        return [source[c, pulse * width : (pulse + 1) * width, lanes]]

    def total(parts):
        value = parts[0]
        for part in parts[1:]:
            value = value + part
        return value

    for tile in range(tiles):
        start = anchors[tile] - tile * TILE_X + LANES
        far = start >= LANES
        amount = jnp.bitwise_and(-start, LANES - 1)
        keep = lane < LANES - jnp.bitwise_and(start, LANES - 1)
        for c in range(2):
            blocks = []
            for kind in (-1, 0, 1, 2):
                block = 2 * tile + kind
                parts = []
                if 0 <= block:
                    parts += [common[c, block * width : (block + 1) * width, :LANES]]
                if kind == -1:
                    parts += take(edge_first, c, block, FIRST_BLOCK, 0)
                if kind < 2:
                    parts += take(edge_low, c, block, 0, 0)
                if kind > -1:
                    parts += take(edge_high, c, block, 2 * STEPS - 2, 0)
                if kind == 2:
                    parts += take(edge_last, c, block, 2 * STEPS, 0)
                if 0 <= block - 1:
                    parts += [common[c, (block - 1) * width : block * width, LANES:]]
                if kind < 1:
                    parts += take(edge_first, c, block - 1, FIRST_BLOCK, 1)
                else:
                    parts += take(edge_high, c, block - 1, 2 * STEPS - 2, 1)
                blocks.append(total(parts))
            near = [jnp.where(far, blocks[k + 1], blocks[k]) for k in range(3)]
            moved = [pltpu.roll(value, amount, 1) for value in near]
            for half in range(2):
                value = jnp.where(keep, moved[half], moved[half + 1])
                out[tile, c, :, half * LANES : (half + 1) * LANES] = value.astype(BF16)


def project(anchors, data, mixer, table, width):
    rows = data.shape[0]
    pulses = rows // width
    tiles = anchors.shape[0]
    beams = mixer.shape[1] // 2
    span = -(-(2 * tiles + 2) * width // 16) * 16 + 16
    vmem = pl.BlockSpec(memory_space=pltpu.VMEM)

    def kernel(*refs):
        project_kernel(*refs, pulses=pulses, tiles=tiles, width=width, beams=beams)

    return pl.pallas_call(
        kernel,
        out_shape=jax.ShapeDtypeStruct((tiles, 2, width, TILE_X), BF16),
        in_specs=[pl.BlockSpec(memory_space=pltpu.SMEM), vmem, vmem, vmem],
        out_specs=vmem,
        scratch_shapes=[
            pltpu.VMEM((rows, 2 * beams), BF16),
            pltpu.VMEM((rows, 2 * beams), BF16),
            pltpu.VMEM((2, span, 2 * LANES), F32),
            pltpu.VMEM((2, rows, 2 * LANES), F32),
            pltpu.VMEM((2, rows, LANES), F32),
            pltpu.VMEM((2, rows, 2 * LANES), F32),
            pltpu.VMEM((2, rows, 2 * LANES), F32),
        ],
        name="project",
    )(anchors, data, mixer, table)


def turn_kernel(data, out):
    count, _, width, pixels = data.shape
    for c in range(2):
        value = data[:, c].reshape(count * width, pixels).astype(F32)
        out[c] = jnp.transpose(value).astype(BF16)


def turn(data):
    count, _, width, pixels = data.shape
    if width % 16:
        return data.transpose(1, 3, 0, 2).reshape(2, pixels, count * width)
    return pl.pallas_call(
        turn_kernel,
        out_shape=jax.ShapeDtypeStruct((2, pixels, count * width), BF16),
        in_specs=[pl.BlockSpec(memory_space=pltpu.VMEM)],
        out_specs=pl.BlockSpec(memory_space=pltpu.VMEM),
        name="turn",
    )(data)


def local(echoes, integer_cell_displacement, fractional_level_label, steering, tile_anchor):
    devices = lax.axis_size("along")
    pulses, bins = echoes.shape[1], echoes.shape[4]
    width = bins // devices
    table, mixer = make_table(steering, pulses)
    sent = compensate(echoes, integer_cell_displacement, fractional_level_label, devices)
    data = lax.all_to_all(sent, "along", 0, 0, tiled=True)
    data = data.reshape(devices * pulses * width, data.shape[-1])
    finished = project(tile_anchor, data, mixer, table, width)
    return turn(lax.all_to_all(finished, "along", 0, 0, tiled=True))


def solution(mesh):
    placed = (
        P(None, ("scene", "along"), None, None, None),
        P(("scene", "along"), None),
        P(("scene", "along"), None),
        P(),
        P("scene"),
    )
    return jax.shard_map(
        local,
        mesh=mesh,
        in_specs=placed,
        out_specs=P(None, ("scene", "along"), None),
        check_vma=False,
    )
```

```python
import math

import jax
import jax.numpy as jnp
import numpy as np
from jax import lax
from jax.experimental import pallas as pl
from jax.experimental.pallas import tpu as pltpu
from jax.sharding import PartitionSpec as P

TILE_X = 256
STEPS = 16
TAPS = 8
SHIFTS = 16
FRACTION_LEVELS = 16
QUAD = 4093
WAVE_FOURTHS = 37
LANES = 128
FIRST_BLOCK = -2
UNITS = STEPS + 2
COARSE = 4
SPREAD = TAPS + COARSE - 1
F32 = jnp.float32
BF16 = jnp.bfloat16
VMEM = pl.BlockSpec(memory_space=pltpu.VMEM)


def near(value):
    return pltpu.with_memory_space_constraint(value, pltpu.VMEM)


def filter_table():
    fraction = np.arange(FRACTION_LEVELS)[:, None] / FRACTION_LEVELS
    place = np.arange(TAPS)[None, :] - (TAPS // 2 - 1) - fraction
    return np.sinc(place) * (0.54 + 0.46 * np.cos(np.pi * place / (TAPS // 2)))


def circle_series():
    angle = np.cos(np.linspace(0, np.pi, 4001)) * np.pi
    odd = np.stack([angle ** (2 * k + 1) for k in range(6)], 1)
    even = np.stack([angle ** (2 * k) for k in range(7)], 1)
    sine = np.linalg.lstsq(odd, np.sin(angle), rcond=None)[0]
    cosine = np.linalg.lstsq(even, np.cos(angle), rcond=None)[0]
    return [float(c) for c in cosine], [float(c) for c in sine]


def horner(series, value):
    total = series[-1]
    for c in reversed(series[:-1]):
        total = total * value + c
    return total


def circle(turns, period, gain=1.0):
    cosine, sine = circle_series()
    angle = turns * (2.0 * math.pi / period)
    power = angle * angle
    return horner([c * gain for c in cosine], power), horner([c * gain for c in sine], power) * angle


def centred(value, period):
    return value - jnp.round(value * (1.0 / period)) * float(period)


def filter_kernel(cells, other_cells, levels, other_levels, echo, other_echo, *rest, chips):
    outs, (moved, turned) = rest[:-2], rest[-2:]
    _, pulses, tx, rx, bins = echo.shape
    chans = tx * rx
    half = bins // 2
    count = 2 * pulses
    me = lax.axis_index("along")
    core = lax.rem(me, 2)
    chip = lax.div(me, 2)

    spread = lax.broadcasted_iota(jnp.int32, (tx, chans), 0) == lax.div(lax.broadcasted_iota(jnp.int32, (tx, chans), 1), rx)
    spread = spread.astype(F32)

    def per_lane(own, other):
        labels = jnp.concatenate([own[...].astype(F32), other[...].astype(F32)], 0)
        return jnp.dot(labels, spread, preferred_element_type=F32)

    cell = per_lane(cells, other_cells)
    level = per_lane(levels, other_levels)
    coarse = jnp.floor(cell * (1.0 / COARSE))
    fine = cell - coarse * COARSE
    table = filter_table()
    weights = []
    for tap in range(TAPS):
        weight = jnp.zeros_like(level)
        for value in range(FRACTION_LEVELS):
            weight = jnp.where(level == float(value), float(table[value, tap]), weight)
        weights.append(weight)
    spread_weights = []
    for place in range(SPREAD):
        total = jnp.zeros_like(level)
        for step in range(COARSE):
            if 0 <= place - step < TAPS:
                total = jnp.where(fine == float(step), weights[place - step], total)
        spread_weights.append(total)
    period = 4 * FRACTION_LEVELS
    turn_cos, turn_sin = circle(centred(WAVE_FOURTHS * (cell * FRACTION_LEVELS + level), period), period)

    span = moved.shape[2]
    steps = SHIFTS // COARSE
    first = SHIFTS // 2 + TAPS // 2 - 1
    row = lax.broadcasted_iota(jnp.int32, (steps * span, bins), 0)
    shift = lax.div(row, span)
    wanted = half * core + row - span * shift - first + COARSE * shift
    select = (lax.broadcasted_iota(jnp.int32, (steps * span, bins), 1) == wanted).astype(F32).astype(BF16)

    for index in range(count):
        source = echo if index < pulses else other_echo
        pick = coarse[index : index + 1]
        for part in range(2):
            rows = source[part, index % pulses].reshape(chans, bins)
            shifted = lax.dot_general(select, rows, (((1,), (1,)), ((), ())), preferred_element_type=F32)
            value = shifted[:span]
            for step in range(1, steps):
                value = jnp.where(pick == float(step), shifted[step * span : (step + 1) * span], value)
            for lane in range(chans // LANES):
                moved[part, lane, :, :] = value[:, lane * LANES : (lane + 1) * LANES]
        place = lax.rem(core + index // pulses, 2) * pulses + index % pulses
        for lane in range(chans // LANES):
            at = slice(lane * LANES, (lane + 1) * LANES)
            taps = [jnp.broadcast_to(w[index : index + 1, at], (8, LANES)) for w in spread_weights]
            lane_cos = jnp.broadcast_to(turn_cos[index : index + 1, at], (8, LANES))
            lane_sin = jnp.broadcast_to(turn_sin[index : index + 1, at], (8, LANES))
            for base in range(0, half, 16):
                reals, imags = [], []
                for begin in (base, base + 8):
                    sums = []
                    for part in range(2):
                        total = taps[0] * moved[part, lane, begin : begin + 8, :]
                        for tap in range(1, SPREAD):
                            total = total + taps[tap] * moved[part, lane, begin + tap : begin + tap + 8, :]
                        sums.append(total)
                    reals.append(sums[0] * lane_cos + sums[1] * lane_sin)
                    imags.append(sums[1] * lane_cos - sums[0] * lane_sin)
                turned[place, base : base + 16, lane * LANES : (lane + 1) * LANES] = jnp.concatenate(reals, 0).astype(BF16)
                turned[place, base : base + 16, chans + lane * LANES : chans + (lane + 1) * LANES] = jnp.concatenate(imags, 0).astype(BF16)
    if len(outs) == 1:
        outs[0][...] = turned[...]
    else:
        width = half // chips
        for step, out in enumerate(outs):
            begin = pl.multiple_of(jnp.bitwise_xor(chip, step) * width, width)
            out[...] = turned[:, pl.ds(begin, width), :]


def compensate(labels, echoes, chips):
    _, pulses, tx, rx, bins = echoes[0].shape
    half, chans = bins // 2, tx * rx
    width = half // chips
    direct = width % 16 == 0
    count = chips if direct else 1

    def kernel(*refs):
        filter_kernel(*refs, chips=chips)

    shape = (2 * pulses, width if direct else half, 2 * chans)
    done = pl.pallas_call(
        kernel,
        out_shape=[pltpu.VMEM(shape, BF16)] * count,
        in_specs=[VMEM] * 6,
        out_specs=[VMEM] * count,
        scratch_shapes=[
            pltpu.VMEM((2, chans // LANES, half + 16, LANES), F32),
            pltpu.VMEM((2 * pulses, half, 2 * chans), BF16),
        ],
        compiler_params=pltpu.CompilerParams(vmem_limit_bytes=24 << 20),
        name="compensate",
    )(*labels, echoes[0], near(echoes[1]))
    if direct:
        return done
    chip = lax.axis_index("along") // 2
    split = done[0].reshape(2 * pulses, chips, width, 2 * chans)
    return [lax.dynamic_index_in_dim(split, jnp.bitwise_xor(chip, k), 1, False) for k in range(chips)]


def table_kernel(steering, table, mixer, *, beams, gain):
    chans = steering.shape[1]
    real, imag = steering[0], steering[1]
    mixer[:chans, :beams] = real
    mixer[:chans, beams:] = imag
    mixer[chans:, :beams] = -imag
    mixer[chans:, beams:] = real
    step = 32
    lane = lax.broadcasted_iota(jnp.int32, (step, LANES), 1).astype(F32) + float(FIRST_BLOCK * LANES)
    offset = centred(lane, QUAD)
    square = centred(offset * offset, QUAD)
    ahead = centred(2.0 * LANES * offset + LANES * LANES, QUAD)
    for row in range(0, beams, step):
        beam = (lax.broadcasted_iota(jnp.int32, (step, LANES), 0) + row).astype(F32)
        beam_square = centred(beam * beam, QUAD)
        beam_next = beam + 1.0
        state = circle(centred(beam_next * square + beam_square * offset, QUAD), QUAD, gain)
        growth = circle(centred(beam_next * ahead + float(LANES) * beam_square, QUAD), QUAD)
        bend_cos, bend_sin = circle(centred(beam_next * float(2 * LANES * LANES % QUAD), QUAD), QUAD)

        def block(index, carry, row=row, bend_cos=bend_cos, bend_sin=bend_sin):
            state_cos, state_sin, growth_cos, growth_sin = carry
            at = pl.ds(pl.multiple_of(index * LANES, LANES), LANES)
            table[row : row + step, at] = state_cos.astype(BF16)
            table[beams + row : beams + row + step, at] = state_sin.astype(BF16)
            return (
                state_cos * growth_cos - state_sin * growth_sin,
                state_cos * growth_sin + state_sin * growth_cos,
                growth_cos * bend_cos - growth_sin * bend_sin,
                growth_cos * bend_sin + growth_sin * bend_cos,
            )

        lax.fori_loop(0, 2 * UNITS, block, (*state, *growth), unroll=4)


def make_table(steering, pulses):
    _, chans, beams = steering.shape
    gain = (STEPS * pulses * beams) ** -0.5

    def kernel(*refs):
        table_kernel(*refs, beams=beams, gain=gain)

    return pl.pallas_call(
        kernel,
        out_shape=(pltpu.VMEM((2 * beams, 2 * UNITS * LANES), BF16), pltpu.VMEM((2 * chans, 2 * beams), BF16)),
        in_specs=[VMEM],
        out_specs=(VMEM, VMEM),
        compiler_params=pltpu.CompilerParams(vmem_limit_bytes=16 << 20),
        cost_estimate=pl.CostEstimate(flops=40 * beams * 2 * UNITS * LANES * 100, transcendentals=0, bytes_accessed=0),
        name="table",
    )(steering)


def project_kernel(anchors, mixer, table, *rest, pulses, tiles, width, beams):
    pieces, (out, data, left, right, common, edge_first, edge_low, edge_high, edge_last) = rest[:-9], rest[-9:]
    rows = pulses * width
    if len(pieces) == 1:
        gathered = pieces[0][...]
    else:
        chip = lax.div(lax.axis_index("along"), 2)
        part = rows // len(pieces)
        for step, piece in enumerate(pieces):
            begin = pl.multiple_of(jnp.bitwise_xor(chip, step) * part, part)
            data[pl.ds(begin, part), :] = piece[...].reshape(part, data.shape[1])
        gathered = data[...]
    formed = jnp.dot(gathered, mixer[...], preferred_element_type=F32)
    real = formed[:, :beams].astype(BF16)
    imag = formed[:, beams:].astype(BF16)
    left[:, :beams] = real
    left[:, beams:] = -imag
    right[:, :beams] = imag
    right[:, beams:] = real
    last_block = 2 * tiles

    def used(first):
        count = min(pulses, last_block - first + 1)
        return min(rows, -(-count * width // 16) * 16)

    def product(first, count):
        unit = (first - FIRST_BLOCK) // 2
        part = table[:, unit * 2 * LANES : (unit + 1) * 2 * LANES]
        return [jnp.dot(side[:count, :], part, preferred_element_type=F32) for side in (left, right)]

    for c, value in enumerate(product(0, rows)):
        edge_low[c, :rows, :] = value[:, :LANES]
        common[c, :rows, :LANES] = jnp.zeros((rows, LANES), F32)
        common[c, :rows, LANES:] = value[:, LANES:]
        common[c, rows:, :] = jnp.zeros((common.shape[1] - rows, 2 * LANES), F32)
    for c, value in enumerate(product(FIRST_BLOCK, rows)):
        edge_first[c] = value
    for first in range(2, 2 * STEPS - 2, 2):
        if first > last_block:
            break
        count = used(first)
        for c, value in enumerate(product(first, count)):
            at = slice(first * width, first * width + count)
            common[c, at, :] = common[c, at, :] + value
    for first, edge in ((2 * STEPS - 2, edge_high), (2 * STEPS, edge_last)):
        if first <= last_block:
            count = used(first)
            for c, value in enumerate(product(first, count)):
                edge[c, :count, :] = value

    lane = lax.broadcasted_iota(jnp.int32, (1, LANES), 1)

    def take(source, c, block, first, half):
        pulse = block - first
        if first > last_block or not 0 <= pulse < pulses:
            return []
        lanes = slice(half * LANES, (half + 1) * LANES)
        return [source[c, pulse * width : (pulse + 1) * width, lanes]]

    def total(parts):
        value = parts[0]
        for part in parts[1:]:
            value = value + part
        return value

    for tile in range(tiles):
        start = anchors[tile] - tile * TILE_X + LANES
        far = start >= LANES
        amount = jnp.bitwise_and(-start, LANES - 1)
        keep = lane < LANES - jnp.bitwise_and(start, LANES - 1)
        for c in range(2):
            blocks = []
            for kind in (-1, 0, 1, 2):
                block = 2 * tile + kind
                parts = []
                if 0 <= block:
                    parts += [common[c, block * width : (block + 1) * width, :LANES]]
                if kind == -1:
                    parts += take(edge_first, c, block, FIRST_BLOCK, 0)
                if kind < 2:
                    parts += take(edge_low, c, block, 0, 0)
                if kind > -1:
                    parts += take(edge_high, c, block, 2 * STEPS - 2, 0)
                if kind == 2:
                    parts += take(edge_last, c, block, 2 * STEPS, 0)
                if 0 <= block - 1:
                    parts += [common[c, (block - 1) * width : block * width, LANES:]]
                if kind < 1:
                    parts += take(edge_first, c, block - 1, FIRST_BLOCK, 1)
                else:
                    parts += take(edge_high, c, block - 1, 2 * STEPS - 2, 1)
                blocks.append(total(parts))
            close = [jnp.where(far, blocks[k + 1], blocks[k]) for k in range(3)]
            moved = [pltpu.roll(value, amount, 1) for value in close]
            for half in range(2):
                value = jnp.where(keep, moved[half], moved[half + 1])
                out[tile, c, :, half * LANES : (half + 1) * LANES] = value.astype(BF16)


def project(anchors, pieces, mixer, table, pulses, width):
    rows = pulses * width
    tiles = anchors.shape[0]
    chans, beams = mixer.shape[0], mixer.shape[1] // 2
    span = -(-(2 * tiles + 2) * width // 16) * 16 + 16

    def kernel(*refs):
        project_kernel(*refs, pulses=pulses, tiles=tiles, width=width, beams=beams)

    return pl.pallas_call(
        kernel,
        out_shape=pltpu.VMEM((tiles, 2, width, TILE_X), BF16),
        in_specs=[pl.BlockSpec(memory_space=pltpu.SMEM)] + [VMEM] * (2 + len(pieces)),
        out_specs=VMEM,
        scratch_shapes=[
            pltpu.VMEM((rows, chans), BF16),
            pltpu.VMEM((rows, 2 * beams), BF16),
            pltpu.VMEM((rows, 2 * beams), BF16),
            pltpu.VMEM((2, span, 2 * LANES), F32),
            pltpu.VMEM((2, rows, 2 * LANES), F32),
            pltpu.VMEM((2, rows, LANES), F32),
            pltpu.VMEM((2, rows, 2 * LANES), F32),
            pltpu.VMEM((2, rows, 2 * LANES), F32),
        ],
        compiler_params=pltpu.CompilerParams(vmem_limit_bytes=24 << 20),
        name="project",
    )(anchors, near(mixer), near(table), *[near(piece) for piece in pieces])


def turn_kernel(data, out):
    count, _, width, pixels = data.shape
    order = [chip * 2 + core for core in range(2) for chip in range(count // 2)]
    same = lax.broadcasted_iota(jnp.int32, (pixels, pixels), 0) == lax.broadcasted_iota(jnp.int32, (pixels, pixels), 1)
    same = same.astype(F32).astype(BF16)
    for c in range(2):
        value = jnp.concatenate([data[source, c] for source in order], 0)
        out[c] = lax.dot_general(same, value, (((1,), (1,)), ((), ())), preferred_element_type=F32).astype(BF16)


def turn(data):
    count, _, width, pixels = data.shape
    if width % 16:
        data = data.reshape(count // 2, 2, 2, width, pixels)
        return data.transpose(2, 4, 1, 0, 3).reshape(2, pixels, count * width)
    return pl.pallas_call(
        turn_kernel,
        out_shape=jax.ShapeDtypeStruct((2, pixels, count * width), BF16),
        in_specs=[VMEM],
        out_specs=VMEM,
        compiler_params=pltpu.CompilerParams(vmem_limit_bytes=16 << 20),
        name="turn",
    )(near(data))


def local(echoes, integer_cell_displacement, fractional_level_label, steering, tile_anchor):
    devices = lax.axis_size("along")
    chips = devices // 2
    pulses, bins = echoes.shape[1], echoes.shape[4]
    width = bins // devices

    def from_pair(value, step):
        return lax.ppermute(value, "along", [(i, i ^ step) for i in range(devices)])

    labels = []
    for label in (integer_cell_displacement, fractional_level_label):
        labels += [label, from_pair(label, 1)]
    other = from_pair(echoes, 1)
    sent = compensate(labels, (echoes, other), chips)
    table, mixer = make_table(steering, pulses)
    pieces = [sent[0]] + [from_pair(sent[k], 2 * k) for k in range(1, chips)]
    if width % 16:
        chip = lax.axis_index("along") // 2
        order = jnp.bitwise_xor(jnp.arange(chips), chip)
        pieces = [jnp.take(jnp.stack(pieces), order, axis=0).reshape(devices * pulses * width, -1)]
    finished = project(tile_anchor, pieces, mixer, table, devices * pulses, width)
    return turn(lax.all_to_all(finished, "along", 0, 0, tiled=True))


def solution(mesh):
    placed = (
        P(None, ("scene", "along"), None, None, None),
        P(("scene", "along"), None),
        P(("scene", "along"), None),
        P(),
        P("scene"),
    )
    return jax.shard_map(
        local,
        mesh=mesh,
        in_specs=placed,
        out_specs=P(None, ("scene", "along"), None),
        check_vma=False,
    )
```

```python
import math

import jax
import jax.numpy as jnp
import numpy as np
from jax import lax
from jax.experimental import pallas as pl
from jax.experimental.pallas import tpu as pltpu
from jax.sharding import PartitionSpec as P


TILE_X = 256
STEPS = 16
TAPS = 8
SHIFTS = 16
FRACTION_LEVELS = 16
QUAD = 4093
WAVE_FOURTHS = 37
LANES = 128
FIRST_BLOCK = -2
UNITS = STEPS + 2
COARSE = 4
SPREAD = TAPS + COARSE - 1
F32 = jnp.float32
BF16 = jnp.bfloat16
VMEM = pl.BlockSpec(memory_space=pltpu.VMEM)
HBM = pl.BlockSpec(memory_space=pltpu.HBM)


def near(value):
    return pltpu.with_memory_space_constraint(value, pltpu.VMEM)


def far(value):
    return pltpu.with_memory_space_constraint(value, pltpu.HBM)


def filter_table():
    fraction = np.arange(FRACTION_LEVELS)[:, None] / FRACTION_LEVELS
    place = np.arange(TAPS)[None, :] - (TAPS // 2 - 1) - fraction
    return np.sinc(place) * (0.54 + 0.46 * np.cos(np.pi * place / (TAPS // 2)))


def circle_series():
    angle = np.cos(np.linspace(0, np.pi, 4001)) * np.pi
    odd = np.stack([angle ** (2 * k + 1) for k in range(6)], 1)
    even = np.stack([angle ** (2 * k) for k in range(7)], 1)
    sine = np.linalg.lstsq(odd, np.sin(angle), rcond=None)[0]
    cosine = np.linalg.lstsq(even, np.cos(angle), rcond=None)[0]
    return [float(c) for c in cosine], [float(c) for c in sine]


def horner(series, value):
    total = series[-1]
    for c in reversed(series[:-1]):
        total = total * value + c
    return total


def circle(turns, period, gain=1.0):
    cosine, sine = circle_series()
    angle = turns * (2.0 * math.pi / period)
    power = angle * angle
    return horner([c * gain for c in cosine], power), horner([c * gain for c in sine], power) * angle


def centred(value, period):
    return value - jnp.round(value * (1.0 / period)) * float(period)


def filter_pulses(cells, levels, echo, moved, store, core):
    _, pulses, tx, rx, bins = echo.shape
    chans = tx * rx
    half = bins // 2

    spread = lax.broadcasted_iota(jnp.int32, (tx, chans), 0) == lax.div(lax.broadcasted_iota(jnp.int32, (tx, chans), 1), rx)
    spread = spread.astype(F32)
    cell = jnp.dot(cells[...].astype(F32), spread, preferred_element_type=F32)
    level = jnp.dot(levels[...].astype(F32), spread, preferred_element_type=F32)
    coarse = jnp.floor(cell * (1.0 / COARSE))
    fine = cell - coarse * COARSE
    table = filter_table()
    weights = []
    for tap in range(TAPS):
        weight = jnp.zeros_like(level)
        for value in range(FRACTION_LEVELS):
            weight = jnp.where(level == float(value), float(table[value, tap]), weight)
        weights.append(weight)
    spread_weights = []
    for place in range(SPREAD):
        total = jnp.zeros_like(level)
        for step in range(COARSE):
            if 0 <= place - step < TAPS:
                total = jnp.where(fine == float(step), weights[place - step], total)
        spread_weights.append(total)
    period = 4 * FRACTION_LEVELS
    turn_cos, turn_sin = circle(centred(WAVE_FOURTHS * (cell * FRACTION_LEVELS + level), period), period)

    span = moved.shape[3]
    steps = SHIFTS // COARSE
    first = SHIFTS // 2 + TAPS // 2 - 1
    row = lax.broadcasted_iota(jnp.int32, (steps * span, bins), 0)
    shift = lax.div(row, span)
    wanted = half * core + row - span * shift - first + COARSE * shift
    select = (lax.broadcasted_iota(jnp.int32, (steps * span, bins), 1) == wanted).astype(F32).astype(BF16)

    for pulse in range(pulses):
        pick = coarse[pulse : pulse + 1]
        for part in range(2):
            rows = echo[part, pulse].reshape(chans, bins)
            shifted = lax.dot_general(select, rows, (((1,), (1,)), ((), ())), preferred_element_type=F32)
            value = shifted[:span]
            for step in range(1, steps):
                value = jnp.where(pick == float(step), shifted[step * span : (step + 1) * span], value)
            for lane in range(chans // LANES):
                moved[pulse, part, lane, :, :] = value[:, lane * LANES : (lane + 1) * LANES]
        for lane in range(chans // LANES):
            at = slice(lane * LANES, (lane + 1) * LANES)
            taps = [jnp.broadcast_to(w[pulse : pulse + 1, at], (8, LANES)) for w in spread_weights]
            lane_cos = jnp.broadcast_to(turn_cos[pulse : pulse + 1, at], (8, LANES))
            lane_sin = jnp.broadcast_to(turn_sin[pulse : pulse + 1, at], (8, LANES))
            for base in range(0, half, 16):
                reals, imags = [], []
                for begin in (base, base + 8):
                    sums = []
                    for part in range(2):
                        total = taps[0] * moved[pulse, part, lane, begin : begin + 8, :]
                        for tap in range(1, SPREAD):
                            total = total + taps[tap] * moved[pulse, part, lane, begin + tap : begin + tap + 8, :]
                        sums.append(total)
                    reals.append(sums[0] * lane_cos + sums[1] * lane_sin)
                    imags.append(sums[1] * lane_cos - sums[0] * lane_sin)
                store(pulse, slice(base, base + 16), at, jnp.concatenate(reals, 0).astype(BF16))
                at_imag = slice(chans + lane * LANES, chans + (lane + 1) * LANES)
                store(pulse, slice(base, base + 16), at_imag, jnp.concatenate(imags, 0).astype(BF16))


def first_kernel(cells, levels, echo, steering, turned, mixer, near_cells, near_levels, near_echo, near_steering, moved, sems):
    copies = [
        pltpu.make_async_copy(source, target, sems.at[index])
        for index, (source, target) in enumerate(
            ((cells, near_cells), (levels, near_levels), (echo, near_echo), (steering, near_steering))
        )
    ]
    for copy in copies:
        copy.start()
    for copy in copies[:3]:
        copy.wait()

    def store(pulse, rows, lanes, value):
        turned[pulse, rows, lanes] = value

    filter_pulses(near_cells, near_levels, near_echo, moved, store, lax.rem(lax.axis_index("along"), 2))
    copies[3].wait()
    _, chans, beams = steering.shape
    real, imag = near_steering[0], near_steering[1]
    mixer[:chans, :beams] = real
    mixer[:chans, beams:] = imag
    mixer[chans:, :beams] = -imag
    mixer[chans:, beams:] = real


def second_kernel(cells, levels, echo, own, *rest, chips):
    outs, (moved, turned) = rest[:-2], rest[-2:]
    pulses = echo.shape[1]
    half = own.shape[1]
    me = lax.axis_index("along")
    core = lax.rem(me, 2)
    chip = lax.div(me, 2)

    def store(pulse, rows, lanes, value):
        turned[pulse, rows, lanes] = value

    filter_pulses(cells, levels, echo, moved, store, core)
    own_place = core * pulses
    other_place = (1 - core) * pulses
    if len(outs) == 1:
        outs[0][pl.ds(own_place, pulses)] = own[...]
        outs[0][pl.ds(other_place, pulses)] = turned[...]
    else:
        width = half // chips
        for step, out in enumerate(outs):
            begin = pl.multiple_of(jnp.bitwise_xor(chip, step) * width, width)
            out[pl.ds(own_place, pulses)] = own[:, pl.ds(begin, width), :]
            out[pl.ds(other_place, pulses)] = turned[:, pl.ds(begin, width), :]


def filter_first(cells, levels, echoes, steering):
    _, pulses, _, _, bins = echoes.shape
    _, chans, beams = steering.shape
    return pl.pallas_call(
        first_kernel,
        out_shape=(pltpu.VMEM((pulses, bins // 2, 2 * chans), BF16), pltpu.VMEM((2 * chans, 2 * beams), BF16)),
        in_specs=[HBM] * 4,
        out_specs=(VMEM, VMEM),
        scratch_shapes=[
            pltpu.VMEM(cells.shape, jnp.int32),
            pltpu.VMEM(levels.shape, jnp.int32),
            pltpu.VMEM(echoes.shape, BF16),
            pltpu.VMEM(steering.shape, BF16),
            pltpu.VMEM((pulses, 2, chans // LANES, bins // 2 + 16, LANES), F32),
            pltpu.SemaphoreType.DMA((4,)),
        ],
        compiler_params=pltpu.CompilerParams(vmem_limit_bytes=16 << 20),
        cost_estimate=pl.CostEstimate(flops=10**8, transcendentals=0, bytes_accessed=0),
        name="filter_first",
    )(far(cells), far(levels), far(echoes), far(steering))


def filter_second(cells, levels, echoes, own, chips):
    _, pulses, tx, rx, bins = echoes.shape
    half, chans = bins // 2, tx * rx
    width = half // chips
    direct = width % 16 == 0
    count = chips if direct else 1

    def kernel(*refs):
        second_kernel(*refs, chips=chips)

    shape = (2 * pulses, width if direct else half, 2 * chans)
    done = pl.pallas_call(
        kernel,
        out_shape=[pltpu.VMEM(shape, BF16)] * count,
        in_specs=[VMEM] * 4,
        out_specs=[VMEM] * count,
        scratch_shapes=[
            pltpu.VMEM((pulses, 2, chans // LANES, half + 16, LANES), F32),
            pltpu.VMEM((pulses, half, 2 * chans), BF16),
        ],
        compiler_params=pltpu.CompilerParams(vmem_limit_bytes=16 << 20),
        name="filter_second",
    )(near(cells), near(levels), near(echoes), near(own))
    if direct:
        return done
    chip = lax.axis_index("along") // 2
    split = done[0].reshape(2 * pulses, chips, width, 2 * chans)
    return [lax.dynamic_index_in_dim(split, jnp.bitwise_xor(chip, k), 1, False) for k in range(chips)]


def table_kernel(table, *, beams, gain):
    step = 32
    lane = lax.broadcasted_iota(jnp.int32, (step, LANES), 1).astype(F32) + float(FIRST_BLOCK * LANES)
    offset = centred(lane, QUAD)
    square = centred(offset * offset, QUAD)
    ahead = centred(2.0 * LANES * offset + LANES * LANES, QUAD)
    for row in range(0, beams, step):
        beam = (lax.broadcasted_iota(jnp.int32, (step, LANES), 0) + row).astype(F32)
        beam_square = centred(beam * beam, QUAD)
        beam_next = beam + 1.0
        state = circle(centred(beam_next * square + beam_square * offset, QUAD), QUAD, gain)
        growth = circle(centred(beam_next * ahead + float(LANES) * beam_square, QUAD), QUAD)
        bend_cos, bend_sin = circle(centred(beam_next * float(2 * LANES * LANES % QUAD), QUAD), QUAD)

        def block(index, carry, row=row, bend_cos=bend_cos, bend_sin=bend_sin):
            state_cos, state_sin, growth_cos, growth_sin = carry
            at = pl.ds(pl.multiple_of(index * LANES, LANES), LANES)
            table[row : row + step, at] = state_cos.astype(BF16)
            table[beams + row : beams + row + step, at] = state_sin.astype(BF16)
            return (
                state_cos * growth_cos - state_sin * growth_sin,
                state_cos * growth_sin + state_sin * growth_cos,
                growth_cos * bend_cos - growth_sin * bend_sin,
                growth_cos * bend_sin + growth_sin * bend_cos,
            )

        lax.fori_loop(0, 2 * UNITS, block, (*state, *growth), unroll=4)


def make_table(beams, pulses):
    gain = (STEPS * pulses * beams) ** -0.5

    def kernel(*refs):
        table_kernel(*refs, beams=beams, gain=gain)

    return pl.pallas_call(
        kernel,
        out_shape=pltpu.VMEM((2 * beams, 2 * UNITS * LANES), BF16),
        in_specs=[],
        out_specs=VMEM,
        compiler_params=pltpu.CompilerParams(vmem_limit_bytes=16 << 20),
        cost_estimate=pl.CostEstimate(flops=40 * beams * 2 * UNITS * LANES * 100, transcendentals=0, bytes_accessed=0),
        name="table",
    )()


def project_kernel(anchors, mixer, table, *rest, pulses, tiles, width, beams):
    pieces, (out, data, left, right, common, edge_first, edge_low, edge_high, edge_last) = rest[:-9], rest[-9:]
    rows = pulses * width
    if len(pieces) == 1:
        gathered = pieces[0][...]
    else:
        chip = lax.div(lax.axis_index("along"), 2)
        part = rows // len(pieces)
        for step, piece in enumerate(pieces):
            begin = pl.multiple_of(jnp.bitwise_xor(chip, step) * part, part)
            data[pl.ds(begin, part), :] = piece[...].reshape(part, data.shape[1])
        gathered = data[...]
    formed = jnp.dot(gathered, mixer[...], preferred_element_type=F32)
    real = formed[:, :beams].astype(BF16)
    imag = formed[:, beams:].astype(BF16)
    left[:, :beams] = real
    left[:, beams:] = -imag
    right[:, :beams] = imag
    right[:, beams:] = real
    last_block = 2 * tiles

    def used(first):
        count = min(pulses, last_block - first + 1)
        return min(rows, -(-count * width // 16) * 16)

    def product(first, count):
        unit = (first - FIRST_BLOCK) // 2
        part = table[:, unit * 2 * LANES : (unit + 1) * 2 * LANES]
        return [jnp.dot(side[:count, :], part, preferred_element_type=F32) for side in (left, right)]

    for c, value in enumerate(product(0, rows)):
        edge_low[c, :rows, :] = value[:, :LANES]
        common[c, :rows, :LANES] = jnp.zeros((rows, LANES), F32)
        common[c, :rows, LANES:] = value[:, LANES:]
        common[c, rows:, :] = jnp.zeros((common.shape[1] - rows, 2 * LANES), F32)
    for c, value in enumerate(product(FIRST_BLOCK, rows)):
        edge_first[c] = value
    for first in range(2, 2 * STEPS - 2, 2):
        if first > last_block:
            break
        count = used(first)
        for c, value in enumerate(product(first, count)):
            at = slice(first * width, first * width + count)
            common[c, at, :] = common[c, at, :] + value
    for first, edge in ((2 * STEPS - 2, edge_high), (2 * STEPS, edge_last)):
        if first <= last_block:
            count = used(first)
            for c, value in enumerate(product(first, count)):
                edge[c, :count, :] = value

    lane = lax.broadcasted_iota(jnp.int32, (1, LANES), 1)

    def take(source, c, block, first, half):
        pulse = block - first
        if first > last_block or not 0 <= pulse < pulses:
            return []
        lanes = slice(half * LANES, (half + 1) * LANES)
        return [source[c, pulse * width : (pulse + 1) * width, lanes]]

    def total(parts):
        value = parts[0]
        for part in parts[1:]:
            value = value + part
        return value

    for tile in range(tiles):
        start = anchors[tile] - tile * TILE_X + LANES
        far = start >= LANES
        amount = jnp.bitwise_and(-start, LANES - 1)
        keep = lane < LANES - jnp.bitwise_and(start, LANES - 1)
        for c in range(2):
            blocks = []
            for kind in (-1, 0, 1, 2):
                block = 2 * tile + kind
                parts = []
                if 0 <= block:
                    parts += [common[c, block * width : (block + 1) * width, :LANES]]
                if kind == -1:
                    parts += take(edge_first, c, block, FIRST_BLOCK, 0)
                if kind < 2:
                    parts += take(edge_low, c, block, 0, 0)
                if kind > -1:
                    parts += take(edge_high, c, block, 2 * STEPS - 2, 0)
                if kind == 2:
                    parts += take(edge_last, c, block, 2 * STEPS, 0)
                if 0 <= block - 1:
                    parts += [common[c, (block - 1) * width : block * width, LANES:]]
                if kind < 1:
                    parts += take(edge_first, c, block - 1, FIRST_BLOCK, 1)
                else:
                    parts += take(edge_high, c, block - 1, 2 * STEPS - 2, 1)
                blocks.append(total(parts))
            close = [jnp.where(far, blocks[k + 1], blocks[k]) for k in range(3)]
            moved = [pltpu.roll(value, amount, 1) for value in close]
            for half in range(2):
                value = jnp.where(keep, moved[half], moved[half + 1])
                out[tile, c, :, half * LANES : (half + 1) * LANES] = value.astype(BF16)


def project(anchors, pieces, mixer, table, pulses, width):
    rows = pulses * width
    tiles = anchors.shape[0]
    chans, beams = mixer.shape[0], mixer.shape[1] // 2
    span = -(-(2 * tiles + 2) * width // 16) * 16 + 16

    def kernel(*refs):
        project_kernel(*refs, pulses=pulses, tiles=tiles, width=width, beams=beams)

    return pl.pallas_call(
        kernel,
        out_shape=pltpu.VMEM((tiles, 2, width, TILE_X), BF16),
        in_specs=[pl.BlockSpec(memory_space=pltpu.SMEM)] + [VMEM] * (2 + len(pieces)),
        out_specs=VMEM,
        scratch_shapes=[
            pltpu.VMEM((rows, chans), BF16),
            pltpu.VMEM((rows, 2 * beams), BF16),
            pltpu.VMEM((rows, 2 * beams), BF16),
            pltpu.VMEM((2, span, 2 * LANES), F32),
            pltpu.VMEM((2, rows, 2 * LANES), F32),
            pltpu.VMEM((2, rows, LANES), F32),
            pltpu.VMEM((2, rows, 2 * LANES), F32),
            pltpu.VMEM((2, rows, 2 * LANES), F32),
        ],
        compiler_params=pltpu.CompilerParams(vmem_limit_bytes=24 << 20),
        name="project",
    )(anchors, near(mixer), near(table), *[near(piece) for piece in pieces])


def turn_kernel(data, out):
    count, _, _, pixels = data.shape
    order = [chip * 2 + core for core in range(2) for chip in range(count // 2)]
    same = lax.broadcasted_iota(jnp.int32, (pixels, pixels), 0) == lax.broadcasted_iota(jnp.int32, (pixels, pixels), 1)
    same = same.astype(F32).astype(BF16)
    for c in range(2):
        value = jnp.concatenate([data[source, c] for source in order], 0)
        out[c] = lax.dot_general(same, value, (((1,), (1,)), ((), ())), preferred_element_type=F32).astype(BF16)


def turn(data):
    count, _, width, pixels = data.shape
    if width % 16:
        data = data.reshape(count // 2, 2, 2, width, pixels)
        return data.transpose(2, 4, 1, 0, 3).reshape(2, pixels, count * width)
    return pl.pallas_call(
        turn_kernel,
        out_shape=jax.ShapeDtypeStruct((2, pixels, count * width), BF16),
        in_specs=[VMEM],
        out_specs=VMEM,
        compiler_params=pltpu.CompilerParams(vmem_limit_bytes=16 << 20),
        name="turn",
    )(near(data))


def far_first(chips):
    order = []
    for bit in reversed(range((chips - 1).bit_length())):
        order += [k for k in range(1 << bit, min(2 << bit, chips))]
    return order


def local(echoes, integer_cell_displacement, fractional_level_label, steering, tile_anchor):
    devices = lax.axis_size("along")
    chips = devices // 2
    pulses, bins = echoes.shape[1], echoes.shape[4]
    width = bins // devices

    def from_pair(value, step):
        return lax.ppermute(value, "along", [(i, i ^ step) for i in range(devices)])

    other_cells, other_levels, other = [
        from_pair(value, 1) for value in (integer_cell_displacement, fractional_level_label, echoes)
    ]
    own, mixer = filter_first(integer_cell_displacement, fractional_level_label, echoes, steering)
    sent = filter_second(other_cells, other_levels, other, own, chips)
    table = make_table(steering.shape[2], pulses)
    pieces = [sent[0]] + [None] * (chips - 1)
    for k in far_first(chips):
        pieces[k] = from_pair(sent[k], 2 * k)
    if width % 16:
        chip = lax.axis_index("along") // 2
        order = jnp.bitwise_xor(jnp.arange(chips), chip)
        pieces = [jnp.take(jnp.stack(pieces), order, axis=0).reshape(devices * pulses * width, -1)]
    finished = project(tile_anchor, pieces, mixer, table, devices * pulses, width)
    return turn(lax.all_to_all(finished, "along", 0, 0, tiled=True))


def solution(mesh):
    placed = (
        P(None, ("scene", "along"), None, None, None),
        P(("scene", "along"), None),
        P(("scene", "along"), None),
        P(),
        P("scene"),
    )
    return jax.shard_map(
        local,
        mesh=mesh,
        in_specs=placed,
        out_specs=P(None, ("scene", "along"), None),
        check_vma=False,
    )
```

```python
import math

import jax
import jax.numpy as jnp
import numpy as np
from jax import lax
from jax.experimental import pallas as pl
from jax.experimental.pallas import tpu as pltpu
from jax.sharding import PartitionSpec as P


TILE_X = 256
STEPS = 16
TAPS = 8
SHIFTS = 16
FRACTION_LEVELS = 16
QUAD = 4093
WAVE_FOURTHS = 37
LANES = 128
FIRST_BLOCK = -2
UNITS = STEPS + 2
COARSE = 4
SPREAD = TAPS + COARSE - 1
F32 = jnp.float32
BF16 = jnp.bfloat16
VMEM = pl.BlockSpec(memory_space=pltpu.VMEM)
HBM = pl.BlockSpec(memory_space=pltpu.HBM)


def near(value):
    return pltpu.with_memory_space_constraint(value, pltpu.VMEM)


def far(value):
    return pltpu.with_memory_space_constraint(value, pltpu.HBM)


def filter_table():
    fraction = np.arange(FRACTION_LEVELS)[:, None] / FRACTION_LEVELS
    place = np.arange(TAPS)[None, :] - (TAPS // 2 - 1) - fraction
    return np.sinc(place) * (0.54 + 0.46 * np.cos(np.pi * place / (TAPS // 2)))


def circle_series():
    angle = np.cos(np.linspace(0, np.pi, 4001)) * np.pi
    odd = np.stack([angle ** (2 * k + 1) for k in range(6)], 1)
    even = np.stack([angle ** (2 * k) for k in range(7)], 1)
    sine = np.linalg.lstsq(odd, np.sin(angle), rcond=None)[0]
    cosine = np.linalg.lstsq(even, np.cos(angle), rcond=None)[0]
    return [float(c) for c in cosine], [float(c) for c in sine]


def horner(series, value):
    total = series[-1]
    for c in reversed(series[:-1]):
        total = total * value + c
    return total


def circle(turns, period, gain=1.0):
    cosine, sine = circle_series()
    angle = turns * (2.0 * math.pi / period)
    power = angle * angle
    return horner([c * gain for c in cosine], power), horner([c * gain for c in sine], power) * angle


def centred(value, period):
    return value - jnp.round(value * (1.0 / period)) * float(period)


def filter_pulses(cells, levels, echo, moved, store, core):
    _, pulses, tx, rx, bins = echo.shape
    chans = tx * rx
    half = bins // 2

    spread = lax.broadcasted_iota(jnp.int32, (tx, chans), 0) == lax.div(lax.broadcasted_iota(jnp.int32, (tx, chans), 1), rx)
    spread = spread.astype(F32)
    cell = jnp.dot(cells[...].astype(F32), spread, preferred_element_type=F32)
    level = jnp.dot(levels[...].astype(F32), spread, preferred_element_type=F32)
    coarse = jnp.floor(cell * (1.0 / COARSE))
    fine = cell - coarse * COARSE
    table = filter_table()
    weights = []
    for tap in range(TAPS):
        weight = jnp.zeros_like(level)
        for value in range(FRACTION_LEVELS):
            weight = jnp.where(level == float(value), float(table[value, tap]), weight)
        weights.append(weight)
    spread_weights = []
    for place in range(SPREAD):
        total = jnp.zeros_like(level)
        for step in range(COARSE):
            if 0 <= place - step < TAPS:
                total = jnp.where(fine == float(step), weights[place - step], total)
        spread_weights.append(total)
    period = 4 * FRACTION_LEVELS
    turn_cos, turn_sin = circle(centred(WAVE_FOURTHS * (cell * FRACTION_LEVELS + level), period), period)

    span = moved.shape[3]
    steps = SHIFTS // COARSE
    first = SHIFTS // 2 + TAPS // 2 - 1
    row = lax.broadcasted_iota(jnp.int32, (steps * span, bins), 0)
    shift = lax.div(row, span)
    wanted = half * core + row - span * shift - first + COARSE * shift
    select = (lax.broadcasted_iota(jnp.int32, (steps * span, bins), 1) == wanted).astype(F32).astype(BF16)

    for pulse in range(pulses):
        pick = coarse[pulse : pulse + 1]
        for part in range(2):
            rows = echo[part, pulse].reshape(chans, bins)
            shifted = lax.dot_general(select, rows, (((1,), (1,)), ((), ())), preferred_element_type=F32)
            value = shifted[:span]
            for step in range(1, steps):
                value = jnp.where(pick == float(step), shifted[step * span : (step + 1) * span], value)
            for lane in range(chans // LANES):
                moved[pulse, part, lane, :, :] = value[:, lane * LANES : (lane + 1) * LANES]
        for lane in range(chans // LANES):
            at = slice(lane * LANES, (lane + 1) * LANES)
            taps = [jnp.broadcast_to(w[pulse : pulse + 1, at], (8, LANES)) for w in spread_weights]
            lane_cos = jnp.broadcast_to(turn_cos[pulse : pulse + 1, at], (8, LANES))
            lane_sin = jnp.broadcast_to(turn_sin[pulse : pulse + 1, at], (8, LANES))
            for base in range(0, half, 16):
                reals, imags = [], []
                for begin in (base, base + 8):
                    sums = []
                    for part in range(2):
                        total = taps[0] * moved[pulse, part, lane, begin : begin + 8, :]
                        for tap in range(1, SPREAD):
                            total = total + taps[tap] * moved[pulse, part, lane, begin + tap : begin + tap + 8, :]
                        sums.append(total)
                    reals.append(sums[0] * lane_cos + sums[1] * lane_sin)
                    imags.append(sums[1] * lane_cos - sums[0] * lane_sin)
                store(pulse, slice(base, base + 16), at, jnp.concatenate(reals, 0).astype(BF16))
                at_imag = slice(chans + lane * LANES, chans + (lane + 1) * LANES)
                store(pulse, slice(base, base + 16), at_imag, jnp.concatenate(imags, 0).astype(BF16))


def first_kernel(cells, levels, echo, steering, turned, mixer, near_cells, near_levels, near_echo, near_steering, moved, sems):
    copies = [
        pltpu.make_async_copy(source, target, sems.at[index])
        for index, (source, target) in enumerate(
            ((cells, near_cells), (levels, near_levels), (echo, near_echo), (steering, near_steering))
        )
    ]
    for copy in copies:
        copy.start()
    for copy in copies[:3]:
        copy.wait()

    def store(pulse, rows, lanes, value):
        turned[pulse, rows, lanes] = value

    filter_pulses(near_cells, near_levels, near_echo, moved, store, lax.rem(lax.axis_index("along"), 2))
    copies[3].wait()
    _, chans, beams = steering.shape
    real, imag = near_steering[0], near_steering[1]
    mixer[:chans, :beams] = real
    mixer[:chans, beams:] = imag
    mixer[chans:, :beams] = -imag
    mixer[chans:, beams:] = real


def second_kernel(cells, levels, echo, own, *rest, group):
    outs, (moved, turned) = rest[:-2], rest[-2:]
    pulses = echo.shape[1]
    half = own.shape[1]
    me = lax.axis_index("along")
    core = lax.rem(me, 2)
    chip = lax.rem(lax.div(me, 2), group)

    def store(pulse, rows, lanes, value):
        turned[pulse, rows, lanes] = value

    filter_pulses(cells, levels, echo, moved, store, core)
    own_place = core * pulses
    other_place = (1 - core) * pulses
    if len(outs) == 1:
        outs[0][pl.ds(own_place, pulses)] = own[...]
        outs[0][pl.ds(other_place, pulses)] = turned[...]
    else:
        width = half // group
        for step, out in enumerate(outs):
            begin = pl.multiple_of(jnp.bitwise_xor(chip, step) * width, width)
            out[pl.ds(own_place, pulses)] = own[:, pl.ds(begin, width), :]
            out[pl.ds(other_place, pulses)] = turned[:, pl.ds(begin, width), :]


def filter_first(cells, levels, echoes, steering):
    _, pulses, _, _, bins = echoes.shape
    _, chans, beams = steering.shape
    return pl.pallas_call(
        first_kernel,
        out_shape=(pltpu.VMEM((pulses, bins // 2, 2 * chans), BF16), pltpu.VMEM((2 * chans, 2 * beams), BF16)),
        in_specs=[HBM] * 4,
        out_specs=(VMEM, VMEM),
        scratch_shapes=[
            pltpu.VMEM(cells.shape, jnp.int32),
            pltpu.VMEM(levels.shape, jnp.int32),
            pltpu.VMEM(echoes.shape, BF16),
            pltpu.VMEM(steering.shape, BF16),
            pltpu.VMEM((pulses, 2, chans // LANES, bins // 2 + 16, LANES), F32),
            pltpu.SemaphoreType.DMA((4,)),
        ],
        compiler_params=pltpu.CompilerParams(vmem_limit_bytes=16 << 20),
        cost_estimate=pl.CostEstimate(flops=10**8, transcendentals=0, bytes_accessed=0),
        name="filter_first",
    )(far(cells), far(levels), far(echoes), far(steering))


def filter_second(cells, levels, echoes, own, group):
    _, pulses, tx, rx, bins = echoes.shape
    half, chans = bins // 2, tx * rx
    width = half // group
    direct = width % 16 == 0
    count = group if direct else 1

    def kernel(*refs):
        second_kernel(*refs, group=group)

    shape = (2 * pulses, width if direct else half, 2 * chans)
    done = pl.pallas_call(
        kernel,
        out_shape=[pltpu.VMEM(shape, BF16)] * count,
        in_specs=[VMEM] * 4,
        out_specs=[VMEM] * count,
        scratch_shapes=[
            pltpu.VMEM((pulses, 2, chans // LANES, half + 16, LANES), F32),
            pltpu.VMEM((pulses, half, 2 * chans), BF16),
        ],
        compiler_params=pltpu.CompilerParams(vmem_limit_bytes=16 << 20),
        name="filter_second",
    )(near(cells), near(levels), near(echoes), near(own))
    if direct:
        return done
    chip = lax.axis_index("along") // 2 % group
    split = done[0].reshape(2 * pulses, group, width, 2 * chans)
    return [lax.dynamic_index_in_dim(split, jnp.bitwise_xor(chip, k), 1, False) for k in range(group)]


def table_kernel(table, *, beams, gain):
    step = 32
    lane = lax.broadcasted_iota(jnp.int32, (step, LANES), 1).astype(F32) + float(FIRST_BLOCK * LANES)
    offset = centred(lane, QUAD)
    square = centred(offset * offset, QUAD)
    ahead = centred(2.0 * LANES * offset + LANES * LANES, QUAD)
    for row in range(0, beams, step):
        beam = (lax.broadcasted_iota(jnp.int32, (step, LANES), 0) + row).astype(F32)
        beam_square = centred(beam * beam, QUAD)
        beam_next = beam + 1.0
        state = circle(centred(beam_next * square + beam_square * offset, QUAD), QUAD, gain)
        growth = circle(centred(beam_next * ahead + float(LANES) * beam_square, QUAD), QUAD)
        bend_cos, bend_sin = circle(centred(beam_next * float(2 * LANES * LANES % QUAD), QUAD), QUAD)

        def block(index, carry, row=row, bend_cos=bend_cos, bend_sin=bend_sin):
            state_cos, state_sin, growth_cos, growth_sin = carry
            at = pl.ds(pl.multiple_of(index * LANES, LANES), LANES)
            table[row : row + step, at] = state_cos.astype(BF16)
            table[beams + row : beams + row + step, at] = state_sin.astype(BF16)
            return (
                state_cos * growth_cos - state_sin * growth_sin,
                state_cos * growth_sin + state_sin * growth_cos,
                growth_cos * bend_cos - growth_sin * bend_sin,
                growth_cos * bend_sin + growth_sin * bend_cos,
            )

        lax.fori_loop(0, 2 * UNITS, block, (*state, *growth), unroll=4)


def make_table(beams, pulses):
    gain = (STEPS * pulses * beams) ** -0.5

    def kernel(*refs):
        table_kernel(*refs, beams=beams, gain=gain)

    return pl.pallas_call(
        kernel,
        out_shape=pltpu.VMEM((2 * beams, 2 * UNITS * LANES), BF16),
        in_specs=[],
        out_specs=VMEM,
        compiler_params=pltpu.CompilerParams(vmem_limit_bytes=16 << 20),
        cost_estimate=pl.CostEstimate(flops=40 * beams * 2 * UNITS * LANES * 100, transcendentals=0, bytes_accessed=0),
        name="table",
    )()


def unit_of(table, first):
    unit = (first - FIRST_BLOCK) // 2
    return table[:, unit * 2 * LANES : (unit + 1) * 2 * LANES]


def tile_window(anchors, tile):
    start = anchors[tile] - tile * TILE_X + LANES
    lane = lax.broadcasted_iota(jnp.int32, (1, LANES), 1)
    within = jnp.bitwise_and(start, LANES - 1)
    return start >= LANES, jnp.bitwise_and(-start, LANES - 1), lane < LANES - within


def store_tile(out, tile, c, blocks, window):
    later, amount, keep = window
    close = [jnp.where(later, blocks[k + 1], blocks[k]) for k in range(3)]
    moved = [pltpu.roll(value, amount, 1) for value in close]
    for half in range(2):
        value = jnp.where(keep, moved[half], moved[half + 1])
        out[tile, c, :, half * LANES : (half + 1) * LANES] = value.astype(BF16)


def form_beams(data, mixer, left, right):
    beams = mixer.shape[1] // 2
    formed = jnp.dot(data, mixer[...], preferred_element_type=F32)
    real = formed[:, :beams].astype(BF16)
    imag = formed[:, beams:].astype(BF16)
    left[:, :beams] = real
    left[:, beams:] = -imag
    right[:, :beams] = imag
    right[:, beams:] = real


def gather_pieces(pieces, data, chip):
    part = data.shape[0] // len(pieces)
    for step, piece in enumerate(pieces):
        begin = pl.multiple_of(jnp.bitwise_xor(chip, step) * part, part)
        data[pl.ds(begin, part), :] = piece[...].reshape(part, data.shape[1])
    return data[...]


def project_tiles(anchors, first_tile, table, left, right, out, common, edge_first, edge_low, edge_high, edge_last,
                  *, pulses, tiles, width):
    rows = pulses * width
    last_block = 2 * tiles

    def used(first):
        count = min(pulses, last_block - first + 1)
        return min(rows, -(-count * width // 16) * 16)

    def product(first, count):
        part = unit_of(table, first)
        return [jnp.dot(side[:count, :], part, preferred_element_type=F32) for side in (left, right)]

    for c, value in enumerate(product(0, rows)):
        edge_low[c, :rows, :] = value[:, :LANES]
        common[c, :rows, :LANES] = jnp.zeros((rows, LANES), F32)
        common[c, :rows, LANES:] = value[:, LANES:]
        common[c, rows:, :] = jnp.zeros((common.shape[1] - rows, 2 * LANES), F32)
    for c, value in enumerate(product(FIRST_BLOCK, rows)):
        edge_first[c] = value
    for first in range(2, 2 * STEPS - 2, 2):
        if first > last_block:
            break
        count = used(first)
        for c, value in enumerate(product(first, count)):
            at = slice(first * width, first * width + count)
            common[c, at, :] = common[c, at, :] + value
    for first, edge in ((2 * STEPS - 2, edge_high), (2 * STEPS, edge_last)):
        if first <= last_block:
            count = used(first)
            for c, value in enumerate(product(first, count)):
                edge[c, :count, :] = value

    def take(source, c, block, first, half):
        pulse = block - first
        if first > last_block or not 0 <= pulse < pulses:
            return []
        lanes = slice(half * LANES, (half + 1) * LANES)
        return [source[c, pulse * width : (pulse + 1) * width, lanes]]

    def total(parts):
        value = parts[0]
        for part in parts[1:]:
            value = value + part
        return value

    for tile in range(tiles):
        window = tile_window(anchors, first_tile + tile)
        for c in range(2):
            blocks = []
            for kind in (-1, 0, 1, 2):
                block = 2 * tile + kind
                parts = []
                if 0 <= block:
                    parts += [common[c, block * width : (block + 1) * width, :LANES]]
                if kind == -1:
                    parts += take(edge_first, c, block, FIRST_BLOCK, 0)
                if kind < 2:
                    parts += take(edge_low, c, block, 0, 0)
                if kind > -1:
                    parts += take(edge_high, c, block, 2 * STEPS - 2, 0)
                if kind == 2:
                    parts += take(edge_last, c, block, 2 * STEPS, 0)
                if 0 <= block - 1:
                    parts += [common[c, (block - 1) * width : block * width, LANES:]]
                if kind < 1:
                    parts += take(edge_first, c, block - 1, FIRST_BLOCK, 1)
                else:
                    parts += take(edge_high, c, block - 1, 2 * STEPS - 2, 1)
                blocks.append(total(parts))
            store_tile(out, tile, c, blocks, window)


def project_kernel(anchors, mixer, table, *rest, pulses, tiles, width):
    pieces, (out, data, left, right, *sums) = rest[:-9], rest[-9:]
    if len(pieces) == 1:
        gathered = pieces[0][...]
    else:
        gathered = gather_pieces(pieces, data, lax.div(lax.axis_index("along"), 2))
    form_beams(gathered, mixer, left, right)
    project_tiles(anchors, 0, table, left, right, out, *sums, pulses=pulses, tiles=tiles, width=width)


def sum_shapes(rows, tiles, width):
    span = -(-(2 * tiles + 2) * width // 16) * 16 + 16
    return [
        pltpu.VMEM((2, span, 2 * LANES), F32),
        pltpu.VMEM((2, rows, 2 * LANES), F32),
        pltpu.VMEM((2, rows, LANES), F32),
        pltpu.VMEM((2, rows, 2 * LANES), F32),
        pltpu.VMEM((2, rows, 2 * LANES), F32),
    ]


def project(anchors, pieces, mixer, table, pulses, width):
    rows = pulses * width
    tiles = anchors.shape[0]
    chans, beams = mixer.shape[0], mixer.shape[1] // 2

    def kernel(*refs):
        project_kernel(*refs, pulses=pulses, tiles=tiles, width=width)

    return pl.pallas_call(
        kernel,
        out_shape=pltpu.VMEM((tiles, 2, width, TILE_X), BF16),
        in_specs=[pl.BlockSpec(memory_space=pltpu.SMEM)] + [VMEM] * (2 + len(pieces)),
        out_specs=VMEM,
        scratch_shapes=[
            pltpu.VMEM((rows, chans), BF16),
            pltpu.VMEM((rows, 2 * beams), BF16),
            pltpu.VMEM((rows, 2 * beams), BF16),
            *sum_shapes(rows, tiles, width),
        ],
        compiler_params=pltpu.CompilerParams(vmem_limit_bytes=24 << 20),
        name="project",
    )(anchors, near(mixer), near(table), *[near(piece) for piece in pieces])


def upper_kernel(anchors, mixer, table, *rest, pulses, tiles, width):
    pieces, (left, right, *sent, data, sums, whole) = rest[: tiles // 2], rest[tiles // 2 :]
    me = lax.axis_index("along")
    core = lax.rem(me, 2)
    group = len(pieces)
    chip = lax.rem(lax.div(me, 2), group)
    form_beams(gather_pieces(pieces, data, chip), mixer, left, right)
    first_block = 2 * tiles - 2
    last_block = 4 * tiles

    @pl.when(me < tiles)
    def _():
        sums[...] = jnp.zeros(sums.shape, F32)
        for first in range(0, last_block + 1, 2):
            low = max(0, first_block - first)
            high = min(pulses - 1, last_block - first)
            rows = slice(low * width, (high + 1) * width)
            at = slice((low + first - first_block) * width, (high + 1 + first - first_block) * width)
            part = unit_of(table, first)
            for c, side in enumerate((left, right)):
                sums[c, at, :] = sums[c, at, :] + jnp.dot(side[rows, :], part, preferred_element_type=F32)
        for tile in range(tiles):
            window = tile_window(anchors, tiles + tile)
            for c in range(2):
                blocks = []
                for kind in (-1, 0, 1, 2):
                    row = (2 * (tiles + tile) + kind - first_block) * width
                    blocks.append(sums[c, row : row + width, :LANES] + sums[c, row - width : row, LANES:])
                store_tile(whole, tile, c, blocks, window)
        deal(whole, sent, chip, core)


def deal(whole, sent, chip, core):
    for place, out in enumerate(sent):
        tile = 2 * jnp.bitwise_xor(chip, place // 2) + jnp.bitwise_xor(core, place % 2)
        out[...] = whole[tile]


def upper_part(anchors, pieces, mixer, table, pulses, width):
    rows = pulses * width
    tiles = anchors.shape[0] // 2
    chans, beams = mixer.shape[0], mixer.shape[1] // 2

    def kernel(*refs):
        upper_kernel(*refs, pulses=pulses, tiles=tiles, width=width)

    side = pltpu.VMEM((rows, 2 * beams), BF16)
    left, right, *sent = pl.pallas_call(
        kernel,
        out_shape=[side, side] + [pltpu.VMEM((2, width, TILE_X), BF16)] * tiles,
        in_specs=[pl.BlockSpec(memory_space=pltpu.SMEM)] + [VMEM] * (2 + len(pieces)),
        out_specs=[VMEM] * (2 + tiles),
        scratch_shapes=[
            pltpu.VMEM((rows, chans), BF16),
            pltpu.VMEM((2, (2 * tiles + 3) * width, 2 * LANES), F32),
            pltpu.VMEM((tiles, 2, width, TILE_X), BF16),
        ],
        compiler_params=pltpu.CompilerParams(vmem_limit_bytes=16 << 20),
        name="upper_part",
    )(anchors, near(mixer), near(table), *[near(piece) for piece in pieces])
    return left, right, sent


def own_kernel(anchors, left, right, table, *rest, pulses, tiles, width, group):
    sent, (whole, *sums) = rest[:-6], rest[-6:]
    me = lax.axis_index("along")
    first_tile = lax.div(me, tiles) * tiles
    project_tiles(anchors, first_tile, table, left, right, whole, *sums, pulses=pulses, tiles=tiles, width=width)
    deal(whole, sent, lax.rem(lax.div(me, 2), group), lax.rem(me, 2))


def own_part(anchors, left, right, table, pulses, width, group):
    rows = pulses * width
    tiles = anchors.shape[0] // 2

    def kernel(*refs):
        own_kernel(*refs, pulses=pulses, tiles=tiles, width=width, group=group)

    return pl.pallas_call(
        kernel,
        out_shape=[pltpu.VMEM((2, width, TILE_X), BF16)] * tiles,
        in_specs=[pl.BlockSpec(memory_space=pltpu.SMEM)] + [VMEM] * 3,
        out_specs=[VMEM] * tiles,
        scratch_shapes=[pltpu.VMEM((tiles, 2, width, TILE_X), BF16), *sum_shapes(rows, tiles, width)],
        compiler_params=pltpu.CompilerParams(vmem_limit_bytes=16 << 20),
        name="own_part",
    )(anchors, near(left), near(right), near(table))


def same_matrix(size):
    same = lax.broadcasted_iota(jnp.int32, (size, size), 0) == lax.broadcasted_iota(jnp.int32, (size, size), 1)
    return same.astype(F32).astype(BF16)


def join_kernel(*refs, group):
    count = 2 * group
    own, lower, (out, scratch) = refs[:count], refs[count : 2 * count], refs[2 * count :]
    _, width, pixels = own[0].shape
    me = lax.axis_index("along")
    core = lax.rem(me, 2)
    chip = lax.rem(lax.div(me, 2), group)
    same = same_matrix(pixels)
    for place in range(count):
        part = jnp.bitwise_xor(core, place % 2) * group + jnp.bitwise_xor(chip, place // 2)
        begin = pl.multiple_of(part * width, width)
        for c in range(2):
            value = own[place][c].astype(F32) + lower[place][c].astype(F32)
            scratch[c, pl.ds(begin, width), :] = value.astype(BF16)
    for c in range(2):
        turned = lax.dot_general(same, scratch[c], (((1,), (1,)), ((), ())), preferred_element_type=F32)
        out[c] = turned.astype(BF16)


def join(own, lower, group):
    _, width, pixels = own[0].shape
    bins = 2 * group * width

    def kernel(*refs):
        join_kernel(*refs, group=group)

    return pl.pallas_call(
        kernel,
        out_shape=jax.ShapeDtypeStruct((2, pixels, bins), BF16),
        in_specs=[VMEM] * (4 * group),
        out_specs=VMEM,
        scratch_shapes=[pltpu.VMEM((2, bins, pixels), BF16)],
        compiler_params=pltpu.CompilerParams(vmem_limit_bytes=16 << 20),
        name="join",
    )(*[near(value) for value in (*own, *lower)])


def turn_kernel(data, out):
    count, _, _, pixels = data.shape
    order = [chip * 2 + core for core in range(2) for chip in range(count // 2)]
    same = same_matrix(pixels)
    for c in range(2):
        value = jnp.concatenate([data[source, c] for source in order], 0)
        out[c] = lax.dot_general(same, value, (((1,), (1,)), ((), ())), preferred_element_type=F32).astype(BF16)


def turn(data):
    count, _, width, pixels = data.shape
    if width % 16:
        data = data.reshape(count // 2, 2, 2, width, pixels)
        return data.transpose(2, 4, 1, 0, 3).reshape(2, pixels, count * width)
    return pl.pallas_call(
        turn_kernel,
        out_shape=jax.ShapeDtypeStruct((2, pixels, count * width), BF16),
        in_specs=[VMEM],
        out_specs=VMEM,
        compiler_params=pltpu.CompilerParams(vmem_limit_bytes=16 << 20),
        name="turn",
    )(near(data))


def far_first(chips):
    order = []
    for bit in reversed(range((chips - 1).bit_length())):
        order += [k for k in range(1 << bit, min(2 << bit, chips))]
    return order


def far_last(chips):
    return far_first(chips)


def in_halves(devices, bins):
    chips = devices // 2
    return 8 <= devices <= STEPS and devices & (devices - 1) == 0 and bins // chips % 16 == 0


def local(echoes, integer_cell_displacement, fractional_level_label, steering, tile_anchor):
    devices = lax.axis_size("along")
    chips = devices // 2
    pulses, bins = echoes.shape[1], echoes.shape[4]
    halves = in_halves(devices, bins)
    group = chips // 2 if halves else chips
    width = bins // (2 * group)

    def exchange(value, step, up=False):
        sources = range(devices // 2 if up else devices)
        return lax.ppermute(value, "along", [(i, i ^ step) for i in sources])

    other_cells, other_levels, other = [
        exchange(value, 1) for value in (integer_cell_displacement, fractional_level_label, echoes)
    ]
    own, mixer = filter_first(integer_cell_displacement, fractional_level_label, echoes, steering)
    sent = filter_second(other_cells, other_levels, other, own, group)
    table = make_table(steering.shape[2], pulses)
    pieces = [sent[0]] + [None] * (group - 1)
    for k in far_first(group):
        pieces[k] = exchange(sent[k], 2 * k)
    if halves:
        left, right, upper = upper_part(tile_anchor, pieces, mixer, table, chips * pulses, width)
        lower = [exchange(upper[k], devices // 2 + k, up=True) for k in range(chips)]
        parts = own_part(tile_anchor, left, right, table, chips * pulses, width, group)
        owned = [parts[0]] + [None] * (chips - 1)
        for k in (*far_last(chips),):
            owned[k] = exchange(parts[k], k)
        return join(owned, lower, group)
    if width % 16:
        chip = lax.axis_index("along") // 2
        order = jnp.bitwise_xor(jnp.arange(chips), chip)
        pieces = [jnp.take(jnp.stack(pieces), order, axis=0).reshape(devices * pulses * width, -1)]
    finished = project(tile_anchor, pieces, mixer, table, devices * pulses, width)
    return turn(lax.all_to_all(finished, "along", 0, 0, tiled=True))


def solution(mesh):
    placed = (
        P(None, ("scene", "along"), None, None, None),
        P(("scene", "along"), None),
        P(("scene", "along"), None),
        P(),
        P("scene"),
    )
    return jax.shard_map(
        local,
        mesh=mesh,
        in_specs=placed,
        out_specs=P(None, ("scene", "along"), None),
        check_vma=False,
    )
```
